32 devices in a mesh: obs: 2 (over y), bt: 4 (over z), freq: 2 (over x), pol: 2 (over core).
Axes of the slice: x: 2, y: 2, z: 4, core: 2. Of those that a mesh axis runs over, the one named last changes fastest.
Arguments:
- gains: float32 [16, 4, 8, 1984], P(('obs', 'bt', 'pol'), 'freq'), parts along dimension 0, may hold values from -3 to 3
- visibilities: bfloat16 [16, 4, 8, 4096], P('obs', 'freq', None, ('bt', 'pol')), parts along dimension 0, may hold values from -6 to 6
- first_station: int32 [8192], P(('obs', 'bt', 'pol')), parts along dimension 0, may hold values from 0 to 61
- second_station: int32 [8192], P(('obs', 'bt', 'pol')), parts along dimension 0, may hold values from 0 to 61, as said below
- filled_row_count: int32 [16], P(('obs', 'bt', 'pol')), parts along dimension 0, may hold values from 256 to 512
- facet_dir: int32 [16], P('obs'), parts along dimension 0, may hold values from 0 to 7, each once
Outputs:
- corrected: bfloat16 [16, 4, 8, 4096], P('obs', 'freq', None, ('bt', 'pol')), parts along dimension 0
The draws below stay inside these ranges and needn't reach their ends.
There are 2 independent parts, one for each index of `obs`. The reference program is written for one: setup_inputs(seed, part) draws one part's arguments, and reference() takes and returns one part's arrays. A program takes and returns all parts, laid end to end along the dimension named above; each array names one. Nothing has to cross between parts.
Inputs may be any that keep to these rules, and one draw needn't show every extreme that they name: In every row second_station differs from first_station. `facet_dir`: each direction names exactly one facet.
All inputs are finite; a program needn't handle non-finite values.
Results may differ from the reference program's by a relative error of at most 0.001.
Values sent between devices are 32-bit elements; how exact they have to be, the bound alone decides.
No kernel may reach another device: no remote copies, remote signals or barrier semaphores. Data moves between devices by JAX's collectives and lax.ppermute only.
A program may use at most 64 MiB of HBM per device.

```python
import jax
import jax.numpy as jnp
from jax import lax

ARRAY_STATIONS = 62
GAIN_SLOT_COUNT = 4
BLOCK_ROW_COUNT = 512
BLOCKS = 8
DIRS = 8
FACETS = 8
CHANS = 4
TIMES = 32
ROWS = 4096


def station_pair(key):
    folded = jax.random.fold_in(key, 17)
    first_key, second_key = jax.random.split(folded)
    first = jax.random.randint(first_key, (ROWS,), 0, ARRAY_STATIONS, dtype=jnp.int32)
    offset = jax.random.randint(second_key, (ROWS,), 1, ARRAY_STATIONS, dtype=jnp.int32)
    return (first, (first + offset) % ARRAY_STATIONS)


def draw_first_station(key, part):
    return station_pair(key)[0]


def draw_second_station(key, part):
    return station_pair(key)[1]


def with_ends(array, stream_key, low, largest):
    longest = array.shape.index(max(array.shape))
    spots = []
    for shift in (0, 1):
        where = [jax.random.randint(jax.random.fold_in(stream_key, axis), (), 0, length) for axis, length in enumerate(array.shape)]
        where[longest] = (where[longest] + shift) % array.shape[longest]
        spots.append(tuple(where))
    return array.at[spots[0]].set(low).at[spots[1]].set(largest)


def levels(rng, shape, pieces, low, largest):
    def one(dim, shards_of):
        heights = jax.random.uniform(jax.random.fold_in(jax.random.fold_in(rng, 6), dim), (shards_of,), jnp.float32, low / len(pieces), largest / len(pieces))
        return jnp.repeat(jnp.exp(heights), shape[dim] // shards_of).reshape((-1,) + (1,) * (len(shape) - dim - 1))

    level = one(*pieces[0])
    for cut in pieces[1:]:
        level = level * one(*cut)
    return level


def centred(own_key, shape, spread, most, cuts=(), kind=jnp.bfloat16):
    level = levels(own_key, shape, cuts, -0.22, 0.18) if cuts else 1.0
    result = jax.random.normal(own_key, shape, jnp.float32) * spread * level
    return jnp.minimum(jnp.maximum(result, -most), most).astype(kind)


def setup_inputs(seed: int = 0, part: int = 0) -> dict:
    streams_of = jax.random.split(jax.random.key(seed), 7)
    part_keys = jax.random.split(jax.random.fold_in(streams_of[6], part), 7)
    gains = centred(part_keys[0], (DIRS, CHANS, 8, TIMES * ARRAY_STATIONS), 0.5, 3.0, ((0, 8), (1, 2)), jnp.float32)
    visibilities = centred(part_keys[1], (FACETS, CHANS, 8, ROWS), 1.0, 6.0, ((1, 2), (3, 8)))
    first_station = draw_first_station(jax.random.fold_in(jax.random.fold_in(streams_of[6], part), 71), part)
    second_station = draw_second_station(jax.random.fold_in(jax.random.fold_in(streams_of[6], part), 71), part)
    filled_row_count = with_ends(jax.random.randint(part_keys[4], (BLOCKS,), BLOCK_ROW_COUNT // 2, BLOCK_ROW_COUNT + 1), jax.random.fold_in(part_keys[4], 1), BLOCK_ROW_COUNT // 2, BLOCK_ROW_COUNT).astype(jnp.int32)
    facet_dir = jax.random.permutation(part_keys[5], DIRS).astype(jnp.int32)
    return dict(gains=gains, visibilities=visibilities, first_station=first_station, second_station=second_station, filled_row_count=filled_row_count, facet_dir=facet_dir)


def entry(values, row_at, col_at):
    return values[..., 2 * row_at + col_at, :], values[..., 4 + 2 * row_at + col_at, :]


def apply_jones(left_matrix, data, right_matrix):
    real_parts = []
    imag_parts = []
    for out_row in (0, 1):
        for out_col in (0, 1):
            total_re = jnp.zeros_like(left_matrix[..., 0, :])
            total_im = jnp.zeros_like(left_matrix[..., 0, :])
            for middle in (0, 1):
                for column in (0, 1):
                    left_re, left_im = entry(left_matrix, out_row, middle)
                    data_re, data_im = entry(data, middle, column)
                    right_re, right_im = entry(right_matrix, out_col, column)
                    prod_re = left_re * data_re - left_im * data_im
                    prod_im = left_re * data_im + left_im * data_re
                    total_re = total_re + prod_re * right_re + prod_im * right_im
                    total_im = total_im + prod_im * right_re - prod_re * right_im
            real_parts.append(total_re)
            imag_parts.append(total_im)
    return jnp.stack(real_parts + imag_parts, axis=-2)


def slot_blend_weight(antenna, block_rows, slots, stations):
    row_ids = jnp.arange(block_rows, dtype=jnp.int32)
    per_slot = block_rows // slots
    row_slot = row_ids // per_slot
    fraction = ((row_ids % per_slot).astype(jnp.float32) + 0.5) / per_slot
    slot_ids = jnp.arange(slots + 1, dtype=jnp.int32)[:, None, None]
    station_ids = jnp.arange(stations, dtype=jnp.int32)[None, :, None]
    time_weight = jnp.where(slot_ids == row_slot[None, None, :], 1.0 - fraction, 0.0 * fraction)
    time_weight = time_weight + jnp.where(slot_ids == row_slot[None, None, :] + 1, fraction, 0.0 * fraction)
    station_mask = (station_ids == antenna[None, None, :]).astype(jnp.float32)
    weights_table = time_weight * station_mask
    return weights_table.reshape((slots + 1) * stations, block_rows)


def apply_correction(gain_window, block_visibilities, first_station_gain, second_station_gain, filled_rows):
    block_rows = block_visibilities.shape[3]
    left_matrix = jnp.einsum("hsxv,va->hsxa", gain_window, slot_blend_weight(first_station_gain, block_rows, GAIN_SLOT_COUNT, ARRAY_STATIONS), precision=lax.Precision.HIGHEST)
    right_matrix = jnp.einsum("hsxv,va->hsxa", gain_window, slot_blend_weight(second_station_gain, block_rows, GAIN_SLOT_COUNT, ARRAY_STATIONS), precision=lax.Precision.HIGHEST)
    product = apply_jones(left_matrix, block_visibilities.astype(jnp.float32), right_matrix)
    live_mask = jnp.arange(block_rows, dtype=jnp.int32) < filled_rows
    return jnp.where(live_mask, product, 0.0 * product).astype(jnp.bfloat16)


def reference(gains, visibilities, first_station, second_station, filled_row_count, facet_dir):
    onehot = (facet_dir[:, None] == jnp.arange(DIRS, dtype=jnp.int32)[None, :]).astype(jnp.float32)
    chosen = jnp.einsum("fd,dckn->fckn", onehot, gains, precision=lax.Precision.HIGHEST)
    final_slot = chosen[..., (TIMES - 1) * ARRAY_STATIONS:]
    extended = jnp.concatenate([chosen, final_slot], axis=3)

    def one_block(block_index):
        gain_window = lax.dynamic_slice_in_dim(extended, block_index * (GAIN_SLOT_COUNT * ARRAY_STATIONS), (GAIN_SLOT_COUNT + 1) * ARRAY_STATIONS, 3)
        block_visibilities = lax.dynamic_slice_in_dim(visibilities, block_index * BLOCK_ROW_COUNT, BLOCK_ROW_COUNT, 3)
        first_station_gain = lax.dynamic_slice_in_dim(first_station, block_index * BLOCK_ROW_COUNT, BLOCK_ROW_COUNT, 0)
        second_station_gain = lax.dynamic_slice_in_dim(second_station, block_index * BLOCK_ROW_COUNT, BLOCK_ROW_COUNT, 0)
        return apply_correction(gain_window, block_visibilities, first_station_gain, second_station_gain, filled_row_count[block_index])

    blocks_out = lax.map(one_block, jnp.arange(BLOCKS, dtype=jnp.int32))
    blocks_out = jnp.moveaxis(blocks_out, 0, 3)
    return blocks_out.reshape(FACETS, CHANS, 8, ROWS)
```

```python
import functools

import jax
import jax.numpy as jnp
from jax import lax
from jax.experimental import pallas as pl
from jax.experimental.pallas import tpu as pltpu
from jax.sharding import PartitionSpec as P

ARRAY_STATIONS = 62
GAIN_SLOT_COUNT = 4
PAD_STATIONS = 64
COMPS = 8
LANES = 128


def pack_kernel(*refs, npol, nbt, chans):
    sources = refs[:npol]
    outs = refs[npol : npol + nbt]
    packed = refs[npol + nbt]
    bt = lax.axis_index("bt")
    pol = lax.axis_index("pol")
    rows = chans * COMPS
    width = sources[0].shape[1]
    slots = width // ARRAY_STATIONS
    lane = lax.broadcasted_iota(jnp.int32, (rows, LANES), 1)
    low = lane < ARRAY_STATIONS
    high = (lane >= PAD_STATIONS) & (lane < PAD_STATIONS + ARRAY_STATIONS)
    pair = 2 * ARRAY_STATIONS
    tail = jnp.zeros((rows, LANES - pair), jnp.float32)
    half = jnp.zeros((rows, LANES - ARRAY_STATIONS), jnp.float32)
    for source_at, source in enumerate(sources):
        values = source[...]
        for at in range(slots // 2):
            near = jnp.concatenate([values[:, at * pair : (at + 1) * pair], tail], axis=1)
            far = pltpu.roll(near, PAD_STATIONS - ARRAY_STATIONS, axis=1)
            packed[source_at, :, at * LANES : (at + 1) * LANES] = jnp.where(
                low, near, jnp.where(high, far, 0.0)
            )
        packed[source_at, :, slots // 2 * LANES :] = jnp.concatenate(
            [values[:, width - ARRAY_STATIONS :], half], axis=1
        )
    own = GAIN_SLOT_COUNT * PAD_STATIONS
    window = own + PAD_STATIONS
    for shift in range(nbt):
        block = lax.rem(bt + shift, nbt) * npol + pol
        start = pl.multiple_of(block * own, LANES)
        for source_at in range(npol):
            wide = packed[source_at, :, pl.ds(start, own + LANES)]
            outs[shift][source_at] = jnp.concatenate(
                [wide[c * COMPS : (c + 1) * COMPS, :window] for c in range(chans)], axis=1
            )


def apply_kernel(*refs, npol, nbt, chans, facets, block_rows):
    facet_dir, filled = refs[:2]
    windows = refs[2 : 2 + nbt]
    vis, first, second, out, facet_at, gathered, wide_vis, wide_out = refs[2 + nbt :]
    bt = lax.axis_index("bt")
    pol = lax.axis_index("pol")
    per_slot = block_rows // GAIN_SLOT_COUNT
    for f in range(facets):
        facet_at[facet_dir[f]] = f
    for slot in range(GAIN_SLOT_COUNT):
        wide_vis[slot] = vis[:, slot * LANES : (slot + 1) * LANES].astype(jnp.float32)
    chunks = gathered.shape[0]
    for shift in range(nbt):
        for source_at in range(npol):
            direction = lax.rem(bt - shift + nbt, nbt) * npol + lax.rem(
                pol - source_at + npol, npol
            )
            row = pl.multiple_of(facet_at[direction] * COMPS, COMPS)
            for chunk in range(chunks):
                gathered[chunk, pl.ds(row, COMPS), :] = windows[shift][
                    source_at, :, chunk * LANES : (chunk + 1) * LANES
                ]
    gains = jnp.concatenate(
        [
            jnp.concatenate(
                [gathered[chunk, pl.ds(k, facets, stride=COMPS), :] for k in range(COMPS)], axis=0
            )
            for chunk in range(chunks)
        ],
        axis=1,
    )
    coarse = gains.astype(jnp.bfloat16)
    fine = (gains - coarse.astype(jnp.float32)).astype(jnp.bfloat16)
    window = (GAIN_SLOT_COUNT + 1) * PAD_STATIONS
    station = lax.broadcasted_iota(jnp.int32, (PAD_STATIONS, per_slot), 0)
    position = lax.broadcasted_iota(jnp.int32, (PAD_STATIONS, per_slot), 1)
    fraction = (position.astype(jnp.float32) + 0.5) / per_slot
    rest = 1.0 - fraction
    place = lax.broadcasted_iota(jnp.int32, (facets, per_slot), 1)
    live_rows = filled[0]

    def table_of(row):
        hit = station == row
        return jnp.concatenate(
            [jnp.where(hit, rest, 0.0), jnp.where(hit, fraction, 0.0)], axis=0
        ).astype(jnp.bfloat16)

    for slot in range(GAIN_SLOT_COUNT):
        table = jnp.concatenate(
            [table_of(first[slot : slot + 1, :]), table_of(second[slot : slot + 1, :])], axis=1
        )
        table = jnp.concatenate([table, table], axis=0)
        parts = []
        for c in range(chans):
            start = c * window + slot * PAD_STATIONS
            stop = start + 2 * PAD_STATIONS
            parts.append(
                jnp.concatenate([coarse[:, start:stop], fine[:, start:stop]], axis=1)
            )
        spread = jnp.dot(
            jnp.concatenate(parts, axis=0), table, preferred_element_type=jnp.float32
        )
        live = place + slot * per_slot < live_rows
        for c in range(chans):

            def side(k, at):
                row = (c * COMPS + k) * facets
                return spread[row : row + facets, at * per_slot : (at + 1) * per_slot]

            def seen(k):
                return wide_vis[slot, pl.ds(c * COMPS + k, facets, stride=chans * COMPS), :]

            left = [(side(k, 0), side(k + 4, 0)) for k in range(4)]
            right = [(side(k, 1), side(k + 4, 1)) for k in range(4)]
            data = [(seen(k), seen(k + 4)) for k in range(4)]
            for r in (0, 1):
                turned = []
                for col in (0, 1):
                    a_re, a_im = left[2 * r]
                    b_re, b_im = left[2 * r + 1]
                    u_re, u_im = data[col]
                    v_re, v_im = data[2 + col]
                    turned.append(
                        (
                            (a_re * u_re - a_im * u_im) + (b_re * v_re - b_im * v_im),
                            (a_re * u_im + a_im * u_re) + (b_re * v_im + b_im * v_re),
                        )
                    )
                (p_re, p_im), (q_re, q_im) = turned
                for oc in (0, 1):
                    x_re, x_im = right[2 * oc]
                    y_re, y_im = right[2 * oc + 1]
                    total_re = (p_re * x_re + p_im * x_im) + (q_re * y_re + q_im * y_im)
                    total_im = (p_im * x_re - p_re * x_im) + (q_im * y_re - q_re * y_im)
                    k = 2 * r + oc
                    rows = chans * COMPS
                    wide_out[slot, pl.ds(c * COMPS + k, facets, stride=rows), :] = jnp.where(
                        live, total_re, 0.0
                    )
                    wide_out[slot, pl.ds(c * COMPS + k + 4, facets, stride=rows), :] = jnp.where(
                        live, total_im, 0.0
                    )
    for slot in range(GAIN_SLOT_COUNT):
        out[:, slot * LANES : (slot + 1) * LANES] = wide_out[slot].astype(jnp.bfloat16)


def vmem():
    return pl.BlockSpec(memory_space=pltpu.VMEM)


def smem():
    return pl.BlockSpec(memory_space=pltpu.SMEM)


def shards(gains, visibilities, first_station, second_station, filled_row_count, facet_dir):
    nbt = lax.axis_size("bt")
    npol = lax.axis_size("pol")
    dirs_here, chans, comps, width = gains.shape
    facets, _, _, block_rows = visibilities.shape
    assert dirs_here == 1 and comps == COMPS
    per_slot = block_rows // GAIN_SLOT_COUNT
    assert per_slot == LANES
    slots = width // ARRAY_STATIONS
    window = chans * (GAIN_SLOT_COUNT + 1) * PAD_STATIONS
    flat = gains.reshape(chans * comps, width)
    sources = [flat] + [
        lax.ppermute(flat, "pol", [(i, (i + s) % npol) for i in range(npol)])
        for s in range(1, npol)
    ]
    outgoing = pl.pallas_call(
        functools.partial(pack_kernel, npol=npol, nbt=nbt, chans=chans),
        out_shape=[jax.ShapeDtypeStruct((npol, comps, window), jnp.float32)] * nbt,
        in_specs=[vmem()] * npol,
        out_specs=[vmem()] * nbt,
        scratch_shapes=[
            pltpu.VMEM((npol, chans * comps, slots * PAD_STATIONS + LANES), jnp.float32)
        ],
        name="pack_windows",
    )(*sources)
    arrived = [outgoing[0]] + [
        lax.ppermute(outgoing[k], "bt", [(i, (i + k) % nbt) for i in range(nbt)])
        for k in range(1, nbt)
    ]
    rows = facets * chans * comps
    corrected = pl.pallas_call(
        functools.partial(
            apply_kernel,
            npol=npol,
            nbt=nbt,
            chans=chans,
            facets=facets,
            block_rows=block_rows,
        ),
        out_shape=jax.ShapeDtypeStruct((rows, block_rows), jnp.bfloat16),
        in_specs=[smem(), smem()] + [vmem()] * (nbt + 3),
        out_specs=vmem(),
        scratch_shapes=[
            pltpu.SMEM((facets,), jnp.int32),
            pltpu.VMEM((window // LANES, facets * comps, LANES), jnp.float32),
            pltpu.VMEM((GAIN_SLOT_COUNT, rows, LANES), jnp.float32),
            pltpu.VMEM((GAIN_SLOT_COUNT, rows, LANES), jnp.float32),
        ],
        name="apply_correction",
    )(
        facet_dir,
        filled_row_count,
        *arrived,
        visibilities.reshape(rows, block_rows),
        first_station.reshape(GAIN_SLOT_COUNT, per_slot),
        second_station.reshape(GAIN_SLOT_COUNT, per_slot),
    )
    return corrected.reshape(visibilities.shape)


def solution(mesh):
    return jax.shard_map(
        shards,
        mesh=mesh,
        in_specs=(
            P(("obs", "bt", "pol"), "freq", None, None),
            P("obs", "freq", None, ("bt", "pol")),
            P(("obs", "bt", "pol")),
            P(("obs", "bt", "pol")),
            P(("obs", "bt", "pol")),
            P("obs"),
        ),
        out_specs=P("obs", "freq", None, ("bt", "pol")),
        check_vma=False,
    )
```

```python
import functools

import jax
import jax.numpy as jnp
from jax import lax
from jax.experimental import pallas as pl
from jax.experimental.pallas import tpu as pltpu
from jax.sharding import PartitionSpec as P


ARRAY_STATIONS = 62
GAIN_SLOT_COUNT = 4
PAD_STATIONS = 64
COMPS = 8
LANES = 128


def pack_kernel(*refs, npol, nbt, chans):
    sources = refs[:npol]
    outs = refs[npol : npol + nbt]
    packed = refs[npol + nbt]
    bt = lax.axis_index("bt")
    pol = lax.axis_index("pol")
    rows = chans * COMPS
    width = sources[0].shape[1]
    slots = width // ARRAY_STATIONS
    lane = lax.broadcasted_iota(jnp.int32, (rows, LANES), 1)
    low = lane < ARRAY_STATIONS
    high = (lane >= PAD_STATIONS) & (lane < PAD_STATIONS + ARRAY_STATIONS)
    pair = 2 * ARRAY_STATIONS
    tail = jnp.zeros((rows, LANES - pair), jnp.float32)
    half = jnp.zeros((rows, LANES - ARRAY_STATIONS), jnp.float32)
    for source_at, source in enumerate(sources):
        values = source[...]
        for at in range(slots // 2):
            near = jnp.concatenate([values[:, at * pair : (at + 1) * pair], tail], axis=1)
            far = pltpu.roll(near, PAD_STATIONS - ARRAY_STATIONS, axis=1)
            packed[source_at, :, at * LANES : (at + 1) * LANES] = jnp.where(
                low, near, jnp.where(high, far, 0.0)
            )
        packed[source_at, :, slots // 2 * LANES :] = jnp.concatenate(
            [values[:, width - ARRAY_STATIONS :], half], axis=1
        )
    own = GAIN_SLOT_COUNT * PAD_STATIONS
    window = own + PAD_STATIONS
    for shift in range(nbt):
        block = lax.rem(bt + shift, nbt) * npol + pol
        start = pl.multiple_of(block * own, LANES)
        for source_at in range(npol):
            wide = packed[source_at, :, pl.ds(start, own + LANES)]
            outs[shift][source_at] = jnp.concatenate(
                [wide[c * COMPS : (c + 1) * COMPS, :window] for c in range(chans)], axis=1
            )


def apply_kernel(*refs, npol, nbt, chans, facets, block_rows):
    facet_dir, filled = refs[:2]
    kept = refs[2]
    downs = refs[3 : 2 + nbt]
    ups = refs[2 + nbt : 1 + 2 * nbt]
    vis, first, second, out, facet_at, gathered, wide_vis, wide_out = refs[1 + 2 * nbt :]
    bt = lax.axis_index("bt")
    pol = lax.axis_index("pol")
    per_slot = block_rows // GAIN_SLOT_COUNT
    for f in range(facets):
        facet_at[facet_dir[f]] = f
    for slot in range(GAIN_SLOT_COUNT):
        wide_vis[slot] = vis[:, slot * LANES : (slot + 1) * LANES].astype(jnp.float32)
    chunks = gathered.shape[0]
    for shift in range(nbt):
        for source_at in range(npol):
            direction = lax.rem(bt - shift + nbt, nbt) * npol + lax.rem(
                pol - source_at + npol, npol
            )
            row = pl.multiple_of(facet_at[direction] * COMPS, COMPS)
            for chunk in range(chunks):
                lanes = slice(chunk * LANES, (chunk + 1) * LANES)
                if shift == 0:
                    piece = kept[source_at, :, lanes]
                else:
                    piece = jnp.where(
                        bt >= shift,
                        ups[shift - 1][source_at, :, lanes],
                        downs[shift - 1][source_at, :, lanes],
                    )
                gathered[chunk, pl.ds(row, COMPS), :] = piece
    gains = jnp.concatenate(
        [
            jnp.concatenate(
                [gathered[chunk, pl.ds(k, facets, stride=COMPS), :] for k in range(COMPS)], axis=0
            )
            for chunk in range(chunks)
        ],
        axis=1,
    )
    coarse = gains.astype(jnp.bfloat16)
    fine = (gains - coarse.astype(jnp.float32)).astype(jnp.bfloat16)
    window = (GAIN_SLOT_COUNT + 1) * PAD_STATIONS
    station = lax.broadcasted_iota(jnp.int32, (PAD_STATIONS, per_slot), 0)
    position = lax.broadcasted_iota(jnp.int32, (PAD_STATIONS, per_slot), 1)
    fraction = (position.astype(jnp.float32) + 0.5) / per_slot
    rest = 1.0 - fraction
    place = lax.broadcasted_iota(jnp.int32, (facets, per_slot), 1)
    live_rows = filled[0]

    def table_of(row):
        hit = station == row
        return jnp.concatenate(
            [jnp.where(hit, rest, 0.0), jnp.where(hit, fraction, 0.0)], axis=0
        ).astype(jnp.bfloat16)

    for slot in range(GAIN_SLOT_COUNT):
        table = jnp.concatenate(
            [table_of(first[slot : slot + 1, :]), table_of(second[slot : slot + 1, :])], axis=1
        )
        table = jnp.concatenate([table, table], axis=0)
        parts = []
        for c in range(chans):
            start = c * window + slot * PAD_STATIONS
            stop = start + 2 * PAD_STATIONS
            parts.append(
                jnp.concatenate([coarse[:, start:stop], fine[:, start:stop]], axis=1)
            )
        spread = jnp.dot(
            jnp.concatenate(parts, axis=0), table, preferred_element_type=jnp.float32
        )
        live = place + slot * per_slot < live_rows
        for c in range(chans):

            def side(k, at):
                row = (c * COMPS + k) * facets
                return spread[row : row + facets, at * per_slot : (at + 1) * per_slot]

            def seen(k):
                return wide_vis[slot, pl.ds(c * COMPS + k, facets, stride=chans * COMPS), :]

            left = [(side(k, 0), side(k + 4, 0)) for k in range(4)]
            right = [(side(k, 1), side(k + 4, 1)) for k in range(4)]
            data = [(seen(k), seen(k + 4)) for k in range(4)]
            for r in (0, 1):
                turned = []
                for col in (0, 1):
                    a_re, a_im = left[2 * r]
                    b_re, b_im = left[2 * r + 1]
                    u_re, u_im = data[col]
                    v_re, v_im = data[2 + col]
                    turned.append(
                        (
                            (a_re * u_re - a_im * u_im) + (b_re * v_re - b_im * v_im),
                            (a_re * u_im + a_im * u_re) + (b_re * v_im + b_im * v_re),
                        )
                    )
                (p_re, p_im), (q_re, q_im) = turned
                for oc in (0, 1):
                    x_re, x_im = right[2 * oc]
                    y_re, y_im = right[2 * oc + 1]
                    total_re = (p_re * x_re + p_im * x_im) + (q_re * y_re + q_im * y_im)
                    total_im = (p_im * x_re - p_re * x_im) + (q_im * y_re - q_re * y_im)
                    k = 2 * r + oc
                    rows = chans * COMPS
                    wide_out[slot, pl.ds(c * COMPS + k, facets, stride=rows), :] = jnp.where(
                        live, total_re, 0.0
                    )
                    wide_out[slot, pl.ds(c * COMPS + k + 4, facets, stride=rows), :] = jnp.where(
                        live, total_im, 0.0
                    )
    for slot in range(GAIN_SLOT_COUNT):
        out[:, slot * LANES : (slot + 1) * LANES] = wide_out[slot].astype(jnp.bfloat16)


def vmem():
    return pl.BlockSpec(memory_space=pltpu.VMEM)


def in_vmem(array):
    return pltpu.with_memory_space_constraint(array, pltpu.VMEM)


def smem():
    return pl.BlockSpec(memory_space=pltpu.SMEM)


def shards(gains, visibilities, first_station, second_station, filled_row_count, facet_dir):
    nbt = lax.axis_size("bt")
    npol = lax.axis_size("pol")
    dirs_here, chans, comps, width = gains.shape
    facets, _, _, block_rows = visibilities.shape
    assert dirs_here == 1 and comps == COMPS
    per_slot = block_rows // GAIN_SLOT_COUNT
    assert per_slot == LANES
    slots = width // ARRAY_STATIONS
    window = chans * (GAIN_SLOT_COUNT + 1) * PAD_STATIONS
    flat = gains.reshape(chans * comps, width)
    sources = [flat] + [
        lax.ppermute(flat, "pol", [(i, (i + s) % npol) for i in range(npol)])
        for s in range(1, npol)
    ]
    outgoing = pl.pallas_call(
        functools.partial(pack_kernel, npol=npol, nbt=nbt, chans=chans),
        out_shape=[pltpu.VMEM((npol, comps, window), jnp.float32)] * nbt,
        in_specs=[vmem()] * npol,
        out_specs=[vmem()] * nbt,
        scratch_shapes=[
            pltpu.VMEM((npol, chans * comps, slots * PAD_STATIONS + LANES), jnp.float32)
        ],
        name="pack_windows",
    )(*[in_vmem(s) for s in sources])
    downs, ups = [], []
    for k in range(1, nbt):
        pairs = [(i, i + k - nbt) for i in range(nbt - k, nbt)]
        downs.append(lax.ppermute(outgoing[k], "bt", pairs))
        pairs = [(i, i + k) for i in range(nbt - k)]
        ups.append(lax.ppermute(outgoing[k], "bt", pairs))
    arrived = [in_vmem(a) for a in [outgoing[0], *downs, *ups]]
    rows = facets * chans * comps
    corrected = pl.pallas_call(
        functools.partial(
            apply_kernel,
            npol=npol,
            nbt=nbt,
            chans=chans,
            facets=facets,
            block_rows=block_rows,
        ),
        out_shape=jax.ShapeDtypeStruct((rows, block_rows), jnp.bfloat16),
        in_specs=[smem(), smem()] + [vmem()] * (2 * nbt + 2),
        out_specs=vmem(),
        scratch_shapes=[
            pltpu.SMEM((facets,), jnp.int32),
            pltpu.VMEM((window // LANES, facets * comps, LANES), jnp.float32),
            pltpu.VMEM((GAIN_SLOT_COUNT, rows, LANES), jnp.float32),
            pltpu.VMEM((GAIN_SLOT_COUNT, rows, LANES), jnp.float32),
        ],
        name="apply_correction",
    )(
        facet_dir,
        filled_row_count,
        *arrived,
        in_vmem(visibilities.reshape(rows, block_rows)),
        in_vmem(first_station.reshape(GAIN_SLOT_COUNT, per_slot)),
        in_vmem(second_station.reshape(GAIN_SLOT_COUNT, per_slot)),
    )
    return corrected.reshape(visibilities.shape)


def solution(mesh):
    return jax.shard_map(
        shards,
        mesh=mesh,
        in_specs=(
            P(("obs", "bt", "pol"), "freq", None, None),
            P("obs", "freq", None, ("bt", "pol")),
            P(("obs", "bt", "pol")),
            P(("obs", "bt", "pol")),
            P(("obs", "bt", "pol")),
            P("obs"),
        ),
        out_specs=P("obs", "freq", None, ("bt", "pol")),
        check_vma=False,
    )
```

```python
import functools

import jax
import jax.numpy as jnp
from jax import lax
from jax.experimental import pallas as pl
from jax.experimental.pallas import tpu as pltpu
from jax.sharding import PartitionSpec as P


ARRAY_STATIONS = 62
GAIN_SLOT_COUNT = 4
PAD_STATIONS = 64
COMPS = 8
LANES = 128


def spread_slots(values, packed):
    rows, width = values.shape
    slots = width // ARRAY_STATIONS
    lane = lax.broadcasted_iota(jnp.int32, (rows, LANES), 1)
    low = lane < ARRAY_STATIONS
    high = (lane >= PAD_STATIONS) & (lane < PAD_STATIONS + ARRAY_STATIONS)
    pair = 2 * ARRAY_STATIONS
    tail = jnp.zeros((rows, LANES - pair), jnp.float32)
    half = jnp.zeros((rows, LANES - ARRAY_STATIONS), jnp.float32)
    for at in range(slots // 2):
        near = jnp.concatenate([values[:, at * pair : (at + 1) * pair], tail], axis=1)
        far = pltpu.roll(near, PAD_STATIONS - ARRAY_STATIONS, axis=1)
        packed[:, at * LANES : (at + 1) * LANES] = jnp.where(
            low, near, jnp.where(high, far, 0.0)
        )
    packed[:, slots // 2 * LANES :] = jnp.concatenate(
        [values[:, width - ARRAY_STATIONS :], half], axis=1
    )


def own_kernel(source, packed):
    spread_slots(source[...], packed)


def pack_kernel(*refs, npol, nbt, chans):
    own = refs[0]
    sources = refs[1:npol]
    outs = refs[npol : npol + nbt]
    scratch = refs[npol + nbt :]
    bt = lax.axis_index("bt")
    pol = lax.axis_index("pol")
    for source, packed in zip(sources, scratch):
        spread_slots(source[...], packed)
    step = GAIN_SLOT_COUNT * PAD_STATIONS
    window = step + PAD_STATIONS
    for shift in range(nbt):
        block = lax.rem(bt + shift, nbt) * npol + pol
        start = pl.multiple_of(block * step, LANES)
        for source_at, packed in enumerate((own, *scratch)):
            wide = packed[:, pl.ds(start, step + LANES)]
            outs[shift][source_at] = jnp.concatenate(
                [wide[c * COMPS : (c + 1) * COMPS, :window] for c in range(chans)], axis=1
            )


def prep_kernel(vis, first, second, tables, wide_vis):
    per_slot = first.shape[1]
    station = lax.broadcasted_iota(jnp.int32, (PAD_STATIONS, per_slot), 0)
    position = lax.broadcasted_iota(jnp.int32, (PAD_STATIONS, per_slot), 1)
    fraction = (position.astype(jnp.float32) + 0.5) / per_slot
    rest = 1.0 - fraction
    for slot in range(GAIN_SLOT_COUNT):
        wide_vis[slot] = vis[:, slot * LANES : (slot + 1) * LANES].astype(jnp.float32)
        for side, rows in enumerate((first, second)):
            hit = station == rows[slot : slot + 1, :]
            tables[slot, :, side * per_slot : (side + 1) * per_slot] = jnp.concatenate(
                [jnp.where(hit, rest, 0.0), jnp.where(hit, fraction, 0.0)], axis=0
            ).astype(jnp.bfloat16)


def apply_kernel(*refs, npol, nbt, chans, facets, block_rows):
    facet_dir, filled = refs[:2]
    windows = refs[2 : 2 + nbt]
    tables, wide_vis, out, facet_at, gathered, wide_out = refs[2 + nbt :]
    bt = lax.axis_index("bt")
    pol = lax.axis_index("pol")
    per_slot = block_rows // GAIN_SLOT_COUNT
    for f in range(facets):
        facet_at[facet_dir[f]] = f
    chunks = gathered.shape[0]
    for shift in range(nbt):
        for source_at in range(npol):
            direction = lax.rem(bt - shift + nbt, nbt) * npol + lax.rem(
                pol - source_at + npol, npol
            )
            row = pl.multiple_of(facet_at[direction] * COMPS, COMPS)
            for chunk in range(chunks):
                lanes = slice(chunk * LANES, (chunk + 1) * LANES)
                piece = windows[shift][source_at, :, lanes]
                gathered[chunk, pl.ds(row, COMPS), :] = piece
    gains = jnp.concatenate(
        [
            jnp.concatenate(
                [gathered[chunk, pl.ds(k, facets, stride=COMPS), :] for k in range(COMPS)], axis=0
            )
            for chunk in range(chunks)
        ],
        axis=1,
    )
    coarse = gains.astype(jnp.bfloat16)
    fine = (gains - coarse.astype(jnp.float32)).astype(jnp.bfloat16)
    window = (GAIN_SLOT_COUNT + 1) * PAD_STATIONS
    place = lax.broadcasted_iota(jnp.int32, (facets, per_slot), 1)
    live_rows = filled[0]

    for slot in range(GAIN_SLOT_COUNT):
        table = tables[slot]
        table = jnp.concatenate([table, table], axis=0)
        parts = []
        for c in range(chans):
            start = c * window + slot * PAD_STATIONS
            stop = start + 2 * PAD_STATIONS
            parts.append(
                jnp.concatenate([coarse[:, start:stop], fine[:, start:stop]], axis=1)
            )
        spread = jnp.dot(
            jnp.concatenate(parts, axis=0), table, preferred_element_type=jnp.float32
        )
        live = place + slot * per_slot < live_rows
        for c in range(chans):

            def side(k, at):
                row = (c * COMPS + k) * facets
                return spread[row : row + facets, at * per_slot : (at + 1) * per_slot]

            def seen(k):
                return wide_vis[slot, pl.ds(c * COMPS + k, facets, stride=chans * COMPS), :]

            left = [(side(k, 0), side(k + 4, 0)) for k in range(4)]
            right = [(side(k, 1), side(k + 4, 1)) for k in range(4)]
            data = [(seen(k), seen(k + 4)) for k in range(4)]
            for r in (0, 1):
                turned = []
                for col in (0, 1):
                    a_re, a_im = left[2 * r]
                    b_re, b_im = left[2 * r + 1]
                    u_re, u_im = data[col]
                    v_re, v_im = data[2 + col]
                    turned.append(
                        (
                            (a_re * u_re - a_im * u_im) + (b_re * v_re - b_im * v_im),
                            (a_re * u_im + a_im * u_re) + (b_re * v_im + b_im * v_re),
                        )
                    )
                (p_re, p_im), (q_re, q_im) = turned
                for oc in (0, 1):
                    x_re, x_im = right[2 * oc]
                    y_re, y_im = right[2 * oc + 1]
                    total_re = (p_re * x_re + p_im * x_im) + (q_re * y_re + q_im * y_im)
                    total_im = (p_im * x_re - p_re * x_im) + (q_im * y_re - q_re * y_im)
                    k = 2 * r + oc
                    rows = chans * COMPS
                    wide_out[slot, pl.ds(c * COMPS + k, facets, stride=rows), :] = jnp.where(
                        live, total_re, 0.0
                    )
                    wide_out[slot, pl.ds(c * COMPS + k + 4, facets, stride=rows), :] = jnp.where(
                        live, total_im, 0.0
                    )
    for slot in range(GAIN_SLOT_COUNT):
        out[:, slot * LANES : (slot + 1) * LANES] = wide_out[slot].astype(jnp.bfloat16)


def vmem():
    return pl.BlockSpec(memory_space=pltpu.VMEM)


def in_vmem(array):
    return pltpu.with_memory_space_constraint(array, pltpu.VMEM)


def smem():
    return pl.BlockSpec(memory_space=pltpu.SMEM)


def shards(gains, visibilities, first_station, second_station, filled_row_count, facet_dir):
    nbt = lax.axis_size("bt")
    npol = lax.axis_size("pol")
    dirs_here, chans, comps, width = gains.shape
    facets, _, _, block_rows = visibilities.shape
    assert dirs_here == 1 and comps == COMPS
    per_slot = block_rows // GAIN_SLOT_COUNT
    assert per_slot == LANES
    slots = width // ARRAY_STATIONS
    window = chans * (GAIN_SLOT_COUNT + 1) * PAD_STATIONS
    flat = gains.reshape(chans * comps, width)
    others = []
    for k in range(1, npol):
        others.append(lax.ppermute(flat, "pol", [(i, (i + k) % npol) for i in range(npol)]))
    packed = (chans * comps, slots * PAD_STATIONS + LANES)
    own = pl.pallas_call(
        own_kernel,
        out_shape=pltpu.VMEM(packed, jnp.float32),
        in_specs=[vmem()],
        out_specs=vmem(),
        name="own_windows",
    )(flat)
    outgoing = pl.pallas_call(
        functools.partial(pack_kernel, npol=npol, nbt=nbt, chans=chans),
        out_shape=[pltpu.VMEM((npol, comps, window), jnp.float32)] * nbt,
        in_specs=[vmem()] * npol,
        out_specs=[vmem()] * nbt,
        scratch_shapes=[pltpu.VMEM(packed, jnp.float32)] * (npol - 1),
        name="pack_windows",
    )(in_vmem(own), *[in_vmem(s) for s in others])
    arrived = [outgoing[0]]
    for k in range(1, nbt):
        arrived.append(lax.ppermute(outgoing[k], "bt", [(i, (i + k) % nbt) for i in range(nbt)]))
    rows = facets * chans * comps
    tables, wide_vis = pl.pallas_call(
        prep_kernel,
        out_shape=[
            pltpu.VMEM((GAIN_SLOT_COUNT, 2 * PAD_STATIONS, 2 * per_slot), jnp.bfloat16),
            pltpu.VMEM((GAIN_SLOT_COUNT, rows, LANES), jnp.float32),
        ],
        in_specs=[vmem()] * 3,
        out_specs=[vmem()] * 2,
        name="prepare",
    )(
        visibilities.reshape(rows, block_rows),
        first_station.reshape(GAIN_SLOT_COUNT, per_slot),
        second_station.reshape(GAIN_SLOT_COUNT, per_slot),
    )
    corrected = pl.pallas_call(
        functools.partial(
            apply_kernel,
            npol=npol,
            nbt=nbt,
            chans=chans,
            facets=facets,
            block_rows=block_rows,
        ),
        out_shape=jax.ShapeDtypeStruct((rows, block_rows), jnp.bfloat16),
        in_specs=[smem(), smem()] + [vmem()] * (nbt + 2),
        out_specs=vmem(),
        scratch_shapes=[
            pltpu.SMEM((facets,), jnp.int32),
            pltpu.VMEM((window // LANES, facets * comps, LANES), jnp.float32),
            pltpu.VMEM((GAIN_SLOT_COUNT, rows, LANES), jnp.float32),
        ],
        name="apply_correction",
    )(
        facet_dir,
        filled_row_count,
        *[in_vmem(a) for a in arrived],
        in_vmem(tables),
        in_vmem(wide_vis),
    )
    return corrected.reshape(visibilities.shape)


def solution(mesh):
    return jax.shard_map(
        shards,
        mesh=mesh,
        in_specs=(
            P(("obs", "bt", "pol"), "freq", None, None),
            P("obs", "freq", None, ("bt", "pol")),
            P(("obs", "bt", "pol")),
            P(("obs", "bt", "pol")),
            P(("obs", "bt", "pol")),
            P("obs"),
        ),
        out_specs=P("obs", "freq", None, ("bt", "pol")),
        check_vma=False,
    )
```

```python
import functools

import jax
import jax.numpy as jnp
from jax import lax
from jax.experimental import pallas as pl
from jax.experimental.pallas import tpu as pltpu
from jax.sharding import PartitionSpec as P


ARRAY_STATIONS = 62
GAIN_SLOT_COUNT = 4
PAD_STATIONS = 64
COMPS = 8
LANES = 128


def spread_slots(values, packed):
    rows, width = values.shape
    slots = width // ARRAY_STATIONS
    lane = lax.broadcasted_iota(jnp.int32, (rows, LANES), 1)
    low = lane < ARRAY_STATIONS
    high = (lane >= PAD_STATIONS) & (lane < PAD_STATIONS + ARRAY_STATIONS)
    pair = 2 * ARRAY_STATIONS
    tail = jnp.zeros((rows, LANES - pair), jnp.float32)
    half = jnp.zeros((rows, LANES - ARRAY_STATIONS), jnp.float32)
    for at in range(slots // 2):
        near = jnp.concatenate([values[:, at * pair : (at + 1) * pair], tail], axis=1)
        far = pltpu.roll(near, PAD_STATIONS - ARRAY_STATIONS, axis=1)
        packed[:, at * LANES : (at + 1) * LANES] = jnp.where(
            low, near, jnp.where(high, far, 0.0)
        )
    packed[:, slots // 2 * LANES :] = jnp.concatenate(
        [values[:, width - ARRAY_STATIONS :], half], axis=1
    )


def own_kernel(source, packed):
    spread_slots(source[...], packed)


def pack_kernel(*refs, npol, nbt, chans):
    own = refs[0]
    sources = refs[1:npol]
    outs = refs[npol : npol + nbt]
    scratch = refs[npol + nbt :]
    bt = lax.axis_index("bt")
    pol = lax.axis_index("pol")
    for source, packed in zip(sources, scratch):
        spread_slots(source[...], packed)
    step = GAIN_SLOT_COUNT * PAD_STATIONS
    window = step + PAD_STATIONS
    for shift in range(nbt):
        block = lax.rem(bt + shift, nbt) * npol + pol
        start = pl.multiple_of(block * step, LANES)
        for source_at, packed in enumerate((own, *scratch)):
            wide = packed[:, pl.ds(start, step + LANES)]
            outs[shift][source_at] = jnp.concatenate(
                [wide[c * COMPS : (c + 1) * COMPS, :window] for c in range(chans)], axis=1
            )


def prep_kernel(facet_dir, filled, vis, first, second, plan, tables, wide_vis):
    facets = facet_dir.shape[0]
    for f in range(facets):
        plan[facet_dir[f]] = f
    plan[facets] = filled[0]
    per_slot = first.shape[1]
    station = lax.broadcasted_iota(jnp.int32, (PAD_STATIONS, per_slot), 0)
    position = lax.broadcasted_iota(jnp.int32, (PAD_STATIONS, per_slot), 1)
    fraction = (position.astype(jnp.float32) + 0.5) / per_slot
    rest = 1.0 - fraction
    for slot in range(GAIN_SLOT_COUNT):
        wide_vis[slot] = vis[:, slot * LANES : (slot + 1) * LANES].astype(jnp.float32)
        for side, rows in enumerate((first, second)):
            hit = station == rows[slot : slot + 1, :]
            tables[slot, :, side * per_slot : (side + 1) * per_slot] = jnp.concatenate(
                [jnp.where(hit, rest, 0.0), jnp.where(hit, fraction, 0.0)], axis=0
            ).astype(jnp.bfloat16)


def apply_kernel(*refs, npol, nbt, chans, facets, block_rows):
    plan = refs[0]
    windows = refs[1 : 1 + nbt]
    tables, wide_vis, out, gathered, wide_out = refs[1 + nbt :]
    bt = lax.axis_index("bt")
    pol = lax.axis_index("pol")
    per_slot = block_rows // GAIN_SLOT_COUNT
    chunks = gathered.shape[0]
    for shift in range(nbt):
        for source_at in range(npol):
            direction = lax.rem(bt - shift + nbt, nbt) * npol + lax.rem(
                pol - source_at + npol, npol
            )
            row = pl.multiple_of(plan[direction] * COMPS, COMPS)
            for chunk in range(chunks):
                lanes = slice(chunk * LANES, (chunk + 1) * LANES)
                piece = windows[shift][source_at, :, lanes]
                gathered[chunk, pl.ds(row, COMPS), :] = piece
    gains = jnp.concatenate(
        [
            jnp.concatenate(
                [gathered[chunk, pl.ds(k, facets, stride=COMPS), :] for k in range(COMPS)], axis=0
            )
            for chunk in range(chunks)
        ],
        axis=1,
    )
    coarse = gains.astype(jnp.bfloat16)
    fine = (gains - coarse.astype(jnp.float32)).astype(jnp.bfloat16)
    window = (GAIN_SLOT_COUNT + 1) * PAD_STATIONS
    place = lax.broadcasted_iota(jnp.int32, (facets, per_slot), 1)
    live_rows = plan[facets]

    for slot in range(GAIN_SLOT_COUNT):
        table = tables[slot]
        table = jnp.concatenate([table, table], axis=0)
        parts = []
        for c in range(chans):
            start = c * window + slot * PAD_STATIONS
            stop = start + 2 * PAD_STATIONS
            parts.append(
                jnp.concatenate([coarse[:, start:stop], fine[:, start:stop]], axis=1)
            )
        spread = jnp.dot(
            jnp.concatenate(parts, axis=0), table, preferred_element_type=jnp.float32
        )
        live = place + slot * per_slot < live_rows
        for c in range(chans):

            def side(k, at):
                row = (c * COMPS + k) * facets
                return spread[row : row + facets, at * per_slot : (at + 1) * per_slot]

            def seen(k):
                return wide_vis[slot, pl.ds(c * COMPS + k, facets, stride=chans * COMPS), :]

            left = [(side(k, 0), side(k + 4, 0)) for k in range(4)]
            right = [(side(k, 1), side(k + 4, 1)) for k in range(4)]
            data = [(seen(k), seen(k + 4)) for k in range(4)]
            for r in (0, 1):
                turned = []
                for col in (0, 1):
                    a_re, a_im = left[2 * r]
                    b_re, b_im = left[2 * r + 1]
                    u_re, u_im = data[col]
                    v_re, v_im = data[2 + col]
                    turned.append(
                        (
                            (a_re * u_re - a_im * u_im) + (b_re * v_re - b_im * v_im),
                            (a_re * u_im + a_im * u_re) + (b_re * v_im + b_im * v_re),
                        )
                    )
                (p_re, p_im), (q_re, q_im) = turned
                for oc in (0, 1):
                    x_re, x_im = right[2 * oc]
                    y_re, y_im = right[2 * oc + 1]
                    total_re = (p_re * x_re + p_im * x_im) + (q_re * y_re + q_im * y_im)
                    total_im = (p_im * x_re - p_re * x_im) + (q_im * y_re - q_re * y_im)
                    k = 2 * r + oc
                    rows = chans * COMPS
                    wide_out[slot, pl.ds(c * COMPS + k, facets, stride=rows), :] = jnp.where(
                        live, total_re, 0.0
                    )
                    wide_out[slot, pl.ds(c * COMPS + k + 4, facets, stride=rows), :] = jnp.where(
                        live, total_im, 0.0
                    )
    for slot in range(GAIN_SLOT_COUNT):
        out[:, slot * LANES : (slot + 1) * LANES] = wide_out[slot].astype(jnp.bfloat16)


def vmem():
    return pl.BlockSpec(memory_space=pltpu.VMEM)


def in_vmem(array):
    return pltpu.with_memory_space_constraint(array, pltpu.VMEM)


def smem():
    return pl.BlockSpec(memory_space=pltpu.SMEM)


def shards(gains, visibilities, first_station, second_station, filled_row_count, facet_dir):
    nbt = lax.axis_size("bt")
    npol = lax.axis_size("pol")
    dirs_here, chans, comps, width = gains.shape
    facets, _, _, block_rows = visibilities.shape
    assert dirs_here == 1 and comps == COMPS
    per_slot = block_rows // GAIN_SLOT_COUNT
    assert per_slot == LANES
    slots = width // ARRAY_STATIONS
    window = chans * (GAIN_SLOT_COUNT + 1) * PAD_STATIONS
    flat = gains.reshape(chans * comps, width)
    others = []
    for k in range(1, npol):
        others.append(lax.ppermute(flat, "pol", [(i, (i + k) % npol) for i in range(npol)]))
    packed = (chans * comps, slots * PAD_STATIONS + LANES)
    own = pl.pallas_call(
        own_kernel,
        out_shape=pltpu.VMEM(packed, jnp.float32),
        in_specs=[vmem()],
        out_specs=vmem(),
        name="own_windows",
    )(flat)
    outgoing = pl.pallas_call(
        functools.partial(pack_kernel, npol=npol, nbt=nbt, chans=chans),
        out_shape=[pltpu.VMEM((npol, comps, window), jnp.float32)] * nbt,
        in_specs=[vmem()] * npol,
        out_specs=[vmem()] * nbt,
        scratch_shapes=[pltpu.VMEM(packed, jnp.float32)] * (npol - 1),
        name="pack_windows",
    )(in_vmem(own), *[in_vmem(s) for s in others])
    arrived = [outgoing[0]]
    for k in range(1, nbt):
        arrived.append(lax.ppermute(outgoing[k], "bt", [(i, (i + k) % nbt) for i in range(nbt)]))
    rows = facets * chans * comps
    plan, tables, wide_vis = pl.pallas_call(
        prep_kernel,
        out_shape=[
            pltpu.SMEM((facets + 1,), jnp.int32),
            pltpu.VMEM((GAIN_SLOT_COUNT, 2 * PAD_STATIONS, 2 * per_slot), jnp.bfloat16),
            pltpu.VMEM((GAIN_SLOT_COUNT, rows, LANES), jnp.float32),
        ],
        in_specs=[smem()] * 2 + [vmem()] * 3,
        out_specs=[smem()] + [vmem()] * 2,
        name="prepare",
    )(
        facet_dir,
        filled_row_count,
        visibilities.reshape(rows, block_rows),
        first_station.reshape(GAIN_SLOT_COUNT, per_slot),
        second_station.reshape(GAIN_SLOT_COUNT, per_slot),
    )
    corrected = pl.pallas_call(
        functools.partial(
            apply_kernel,
            npol=npol,
            nbt=nbt,
            chans=chans,
            facets=facets,
            block_rows=block_rows,
        ),
        out_shape=jax.ShapeDtypeStruct((rows, block_rows), jnp.bfloat16),
        in_specs=[smem()] + [vmem()] * (nbt + 2),
        out_specs=vmem(),
        scratch_shapes=[
            pltpu.VMEM((window // LANES, facets * comps, LANES), jnp.float32),
            pltpu.VMEM((GAIN_SLOT_COUNT, rows, LANES), jnp.float32),
        ],
        name="apply_correction",
    )(
        pltpu.with_memory_space_constraint(plan, pltpu.SMEM),
        *[in_vmem(a) for a in arrived],
        in_vmem(tables),
        in_vmem(wide_vis),
    )
    return corrected.reshape(visibilities.shape)


def solution(mesh):
    return jax.shard_map(
        shards,
        mesh=mesh,
        in_specs=(
            P(("obs", "bt", "pol"), "freq", None, None),
            P("obs", "freq", None, ("bt", "pol")),
            P(("obs", "bt", "pol")),
            P(("obs", "bt", "pol")),
            P(("obs", "bt", "pol")),
            P("obs"),
        ),
        out_specs=P("obs", "freq", None, ("bt", "pol")),
        check_vma=False,
    )
```

```python
import functools

import jax
import jax.numpy as jnp
from jax import lax
from jax.experimental import pallas as pl
from jax.experimental.pallas import tpu as pltpu
from jax.sharding import PartitionSpec as P


ARRAY_STATIONS = 62
GAIN_SLOT_COUNT = 4
PAD_STATIONS = 64
COMPS = 8
LANES = 128


def spread_slots(values, packed):
    rows, width = values.shape
    slots = width // ARRAY_STATIONS
    lane = lax.broadcasted_iota(jnp.int32, (rows, LANES), 1)
    low = lane < ARRAY_STATIONS
    high = (lane >= PAD_STATIONS) & (lane < PAD_STATIONS + ARRAY_STATIONS)
    pair = 2 * ARRAY_STATIONS
    tail = jnp.zeros((rows, LANES - pair), jnp.float32)
    half = jnp.zeros((rows, LANES - ARRAY_STATIONS), jnp.float32)
    for at in range(slots // 2):
        near = jnp.concatenate([values[:, at * pair : (at + 1) * pair], tail], axis=1)
        far = pltpu.roll(near, PAD_STATIONS - ARRAY_STATIONS, axis=1)
        packed[:, at * LANES : (at + 1) * LANES] = jnp.where(
            low, near, jnp.where(high, far, 0.0)
        )
    packed[:, slots // 2 * LANES :] = jnp.concatenate(
        [values[:, width - ARRAY_STATIONS :], half], axis=1
    )


def window_of(packed, block, chans):
    step = GAIN_SLOT_COUNT * PAD_STATIONS
    wide = packed[:, pl.ds(pl.multiple_of(block * step, LANES), step + LANES)]
    return jnp.concatenate(
        [wide[c * COMPS : (c + 1) * COMPS, : step + PAD_STATIONS] for c in range(chans)], axis=1
    )


def own_kernel(source, packed, lead, *, npol, nbt, chans):
    bt = lax.axis_index("bt")
    pol = lax.axis_index("pol")
    spread_slots(source[...], packed)
    for s in range(npol):
        block = lax.rem(bt + 1, nbt) * npol + lax.rem(pol + s, npol)
        lead[s] = window_of(packed, block, chans)


def pack_kernel(*refs, npol, nbt, chans):
    own = refs[0]
    sources = refs[1:npol]
    outs = refs[npol : npol + nbt - 1]
    scratch = refs[npol + nbt - 1 :]
    bt = lax.axis_index("bt")
    pol = lax.axis_index("pol")
    for source, packed in zip(sources, scratch):
        spread_slots(source[...], packed)
    for out, shift in zip(outs, [0, *range(2, nbt)]):
        block = lax.rem(bt + shift, nbt) * npol + pol
        for source_at, packed in enumerate((own, *scratch)):
            out[source_at] = window_of(packed, block, chans)


def prep_kernel(facet_dir, filled, vis, first, second, plan, tables, wide_vis):
    facets = facet_dir.shape[0]
    for f in range(facets):
        plan[facet_dir[f]] = f
    plan[facets] = filled[0]
    per_slot = first.shape[1]
    station = lax.broadcasted_iota(jnp.int32, (PAD_STATIONS, per_slot), 0)
    position = lax.broadcasted_iota(jnp.int32, (PAD_STATIONS, per_slot), 1)
    fraction = (position.astype(jnp.float32) + 0.5) / per_slot
    rest = 1.0 - fraction
    for slot in range(GAIN_SLOT_COUNT):
        wide_vis[slot] = vis[:, slot * LANES : (slot + 1) * LANES].astype(jnp.float32)
        for side, rows in enumerate((first, second)):
            hit = station == rows[slot : slot + 1, :]
            tables[slot, :, side * per_slot : (side + 1) * per_slot] = jnp.concatenate(
                [jnp.where(hit, rest, 0.0), jnp.where(hit, fraction, 0.0)], axis=0
            ).astype(jnp.bfloat16)


def apply_kernel(*refs, npol, nbt, chans, facets, block_rows):
    plan = refs[0]
    windows = refs[1 : 1 + nbt]
    late = refs[1 + nbt : nbt + npol]
    tables, wide_vis, out, gathered, wide_out = refs[nbt + npol :]
    bt = lax.axis_index("bt")
    pol = lax.axis_index("pol")
    per_slot = block_rows // GAIN_SLOT_COUNT
    chunks = gathered.shape[0]
    for shift in range(nbt):
        for source_at in range(npol):
            direction = lax.rem(bt - shift + nbt, nbt) * npol + lax.rem(
                pol - source_at + npol, npol
            )
            row = pl.multiple_of(plan[direction] * COMPS, COMPS)
            for chunk in range(chunks):
                lanes = slice(chunk * LANES, (chunk + 1) * LANES)
                if shift == 1 and source_at:
                    piece = late[source_at - 1][:, lanes]
                else:
                    piece = windows[shift][source_at, :, lanes]
                gathered[chunk, pl.ds(row, COMPS), :] = piece
    gains = jnp.concatenate(
        [
            jnp.concatenate(
                [gathered[chunk, pl.ds(k, facets, stride=COMPS), :] for k in range(COMPS)], axis=0
            )
            for chunk in range(chunks)
        ],
        axis=1,
    )
    coarse = gains.astype(jnp.bfloat16)
    fine = (gains - coarse.astype(jnp.float32)).astype(jnp.bfloat16)
    window = (GAIN_SLOT_COUNT + 1) * PAD_STATIONS
    place = lax.broadcasted_iota(jnp.int32, (facets, per_slot), 1)
    live_rows = plan[facets]

    for slot in range(GAIN_SLOT_COUNT):
        table = tables[slot]
        table = jnp.concatenate([table, table], axis=0)
        parts = []
        for c in range(chans):
            start = c * window + slot * PAD_STATIONS
            stop = start + 2 * PAD_STATIONS
            parts.append(
                jnp.concatenate([coarse[:, start:stop], fine[:, start:stop]], axis=1)
            )
        spread = jnp.dot(
            jnp.concatenate(parts, axis=0), table, preferred_element_type=jnp.float32
        )
        live = place + slot * per_slot < live_rows
        for c in range(chans):

            def side(k, at):
                row = (c * COMPS + k) * facets
                return spread[row : row + facets, at * per_slot : (at + 1) * per_slot]

            def seen(k):
                return wide_vis[slot, pl.ds(c * COMPS + k, facets, stride=chans * COMPS), :]

            left = [(side(k, 0), side(k + 4, 0)) for k in range(4)]
            right = [(side(k, 1), side(k + 4, 1)) for k in range(4)]
            data = [(seen(k), seen(k + 4)) for k in range(4)]
            for r in (0, 1):
                turned = []
                for col in (0, 1):
                    a_re, a_im = left[2 * r]
                    b_re, b_im = left[2 * r + 1]
                    u_re, u_im = data[col]
                    v_re, v_im = data[2 + col]
                    turned.append(
                        (
                            (a_re * u_re - a_im * u_im) + (b_re * v_re - b_im * v_im),
                            (a_re * u_im + a_im * u_re) + (b_re * v_im + b_im * v_re),
                        )
                    )
                (p_re, p_im), (q_re, q_im) = turned
                for oc in (0, 1):
                    x_re, x_im = right[2 * oc]
                    y_re, y_im = right[2 * oc + 1]
                    total_re = (p_re * x_re + p_im * x_im) + (q_re * y_re + q_im * y_im)
                    total_im = (p_im * x_re - p_re * x_im) + (q_im * y_re - q_re * y_im)
                    k = 2 * r + oc
                    rows = chans * COMPS
                    wide_out[slot, pl.ds(c * COMPS + k, facets, stride=rows), :] = jnp.where(
                        live, total_re, 0.0
                    )
                    wide_out[slot, pl.ds(c * COMPS + k + 4, facets, stride=rows), :] = jnp.where(
                        live, total_im, 0.0
                    )
    for slot in range(GAIN_SLOT_COUNT):
        out[:, slot * LANES : (slot + 1) * LANES] = wide_out[slot].astype(jnp.bfloat16)


def vmem():
    return pl.BlockSpec(memory_space=pltpu.VMEM)


def in_vmem(array):
    return pltpu.with_memory_space_constraint(array, pltpu.VMEM)


def smem():
    return pl.BlockSpec(memory_space=pltpu.SMEM)


def shards(gains, visibilities, first_station, second_station, filled_row_count, facet_dir):
    nbt = lax.axis_size("bt")
    npol = lax.axis_size("pol")
    dirs_here, chans, comps, width = gains.shape
    facets, _, _, block_rows = visibilities.shape
    assert dirs_here == 1 and comps == COMPS
    per_slot = block_rows // GAIN_SLOT_COUNT
    assert per_slot == LANES
    slots = width // ARRAY_STATIONS
    window = chans * (GAIN_SLOT_COUNT + 1) * PAD_STATIONS
    flat = gains.reshape(chans * comps, width)
    others = []
    for k in range(1, npol):
        others.append(lax.ppermute(flat, "pol", [(i, (i + k) % npol) for i in range(npol)]))
    packed = (chans * comps, slots * PAD_STATIONS + LANES)
    own, lead = pl.pallas_call(
        functools.partial(own_kernel, npol=npol, nbt=nbt, chans=chans),
        out_shape=[pltpu.VMEM(packed, jnp.float32), pltpu.VMEM((npol, comps, window), jnp.float32)],
        in_specs=[vmem()],
        out_specs=[vmem()] * 2,
        name="own_windows",
    )(flat)
    outgoing = pl.pallas_call(
        functools.partial(pack_kernel, npol=npol, nbt=nbt, chans=chans),
        out_shape=[pltpu.VMEM((npol, comps, window), jnp.float32)] * (nbt - 1),
        in_specs=[vmem()] * npol,
        out_specs=[vmem()] * (nbt - 1),
        scratch_shapes=[pltpu.VMEM(packed, jnp.float32)] * (npol - 1),
        name="pack_windows",
    )(in_vmem(own), *[in_vmem(s) for s in others])
    outgoing = [outgoing[0], lead, *outgoing[1:]]
    arrived = [outgoing[0]]
    for k in range(1, nbt):
        arrived.append(lax.ppermute(outgoing[k], "bt", [(i, (i + k) % nbt) for i in range(nbt)]))
    late = []
    for k in range(1, npol):
        late.append(lax.ppermute(arrived[1][k], "pol", [(i, (i + k) % npol) for i in range(npol)]))
    rows = facets * chans * comps
    plan, tables, wide_vis = pl.pallas_call(
        prep_kernel,
        out_shape=[
            pltpu.SMEM((facets + 1,), jnp.int32),
            pltpu.VMEM((GAIN_SLOT_COUNT, 2 * PAD_STATIONS, 2 * per_slot), jnp.bfloat16),
            pltpu.VMEM((GAIN_SLOT_COUNT, rows, LANES), jnp.float32),
        ],
        in_specs=[smem()] * 2 + [vmem()] * 3,
        out_specs=[smem()] + [vmem()] * 2,
        name="prepare",
    )(
        facet_dir,
        filled_row_count,
        visibilities.reshape(rows, block_rows),
        first_station.reshape(GAIN_SLOT_COUNT, per_slot),
        second_station.reshape(GAIN_SLOT_COUNT, per_slot),
    )
    corrected = pl.pallas_call(
        functools.partial(
            apply_kernel,
            npol=npol,
            nbt=nbt,
            chans=chans,
            facets=facets,
            block_rows=block_rows,
        ),
        out_shape=jax.ShapeDtypeStruct((rows, block_rows), jnp.bfloat16),
        in_specs=[smem()] + [vmem()] * (nbt + npol + 1),
        out_specs=vmem(),
        scratch_shapes=[
            pltpu.VMEM((window // LANES, facets * comps, LANES), jnp.float32),
            pltpu.VMEM((GAIN_SLOT_COUNT, rows, LANES), jnp.float32),
        ],
        name="apply_correction",
    )(
        pltpu.with_memory_space_constraint(plan, pltpu.SMEM),
        *[in_vmem(a) for a in arrived + late],
        in_vmem(tables),
        in_vmem(wide_vis),
    )
    return corrected.reshape(visibilities.shape)


def solution(mesh):
    return jax.shard_map(
        shards,
        mesh=mesh,
        in_specs=(
            P(("obs", "bt", "pol"), "freq", None, None),
            P("obs", "freq", None, ("bt", "pol")),
            P(("obs", "bt", "pol")),
            P(("obs", "bt", "pol")),
            P(("obs", "bt", "pol")),
            P("obs"),
        ),
        out_specs=P("obs", "freq", None, ("bt", "pol")),
        check_vma=False,
    )
```
